128 devices in a mesh: col: 2 (over core), row: 64 (over z, y, x).
Axes of the slice: x: 4, y: 4, z: 4, core: 2. Of those that a mesh axis runs over, the one named last changes fastest.
Arguments:
- mask: int32 [262144, 1024], P('row', 'col')
- user_emb: bfloat16 [262144, 64], P(('row', 'col'))
- item_emb: bfloat16 [1024, 64], P(('col', 'row'))
- queries: int32 [1024], replicated
Outputs:
- output 1: bfloat16 [262144, 64], P(('row', 'col'))
- output 2: bfloat16 [1024, 64], P(('col', 'row'))
- output 3: float32 [1024, 1024], P(None, ('col', 'row'))
All inputs are finite; a program needn't handle non-finite values.
Results may differ from the reference program's by a relative error of at most 0.00541896.
Values are sent between devices in bfloat16 or wider.
A program may use at most 1 GiB of HBM per device.

```python
import jax
import jax.numpy as jnp
from jax import lax

USERS = 262144
ITEMS = 1024
EMB = 64
LAYERS = 3
QUERIES = 1024


def draw_mask(key):
    k_noise, k_rows, k_cols = jax.random.split(key, 3)
    row_level = jax.random.randint(k_rows, (USERS,), 4, 33)
    col_level = jax.random.randint(k_cols, (ITEMS,), 4, 33)
    noise = jax.random.randint(k_noise, (USERS, ITEMS), 0, 1024)
    return (noise < row_level[:, None] * col_level[None, :]).astype(jnp.int32)


def setup_inputs(seed: int = 0) -> dict:
    key = jax.random.key(seed)
    k_mask, k_user, k_item, k_umean, k_imean, k_query = jax.random.split(key, 6)
    scale = EMB ** -0.25
    user_mean = jax.random.normal(k_umean, (EMB,), jnp.float32)
    item_mean = jax.random.normal(k_imean, (EMB,), jnp.float32)
    user_emb = ((jax.random.normal(k_user, (USERS, EMB), jnp.float32) + user_mean[None, :]) * scale).astype(jnp.bfloat16)
    item_emb = ((jax.random.normal(k_item, (ITEMS, EMB), jnp.float32) + item_mean[None, :]) * scale).astype(jnp.bfloat16)
    queries = jax.random.randint(k_query, (QUERIES,), 0, USERS).astype(jnp.int32)
    return {'mask': draw_mask(k_mask), 'user_emb': user_emb, 'item_emb': item_emb, 'queries': queries}


def norm_adjacency(mask):
    deg_user = jnp.maximum(jnp.sum(mask, axis=1), 1)
    deg_item = jnp.maximum(jnp.sum(mask, axis=0), 1)
    inv_user = lax.rsqrt(deg_user.astype(jnp.float32))
    inv_item = lax.rsqrt(deg_item.astype(jnp.float32))
    return (inv_user[:, None] * mask.astype(jnp.float32) * inv_item[None, :]).astype(jnp.bfloat16)


def reference(mask, user_emb, item_emb, queries):
    norm_adj = norm_adjacency(mask)

    def one_layer(carried, unused):
        user_cur, item_cur, user_sum, item_sum = carried
        user_next = jnp.dot(norm_adj, item_cur, preferred_element_type=jnp.float32).astype(jnp.bfloat16)
        item_next = lax.dot_general(norm_adj, user_cur, (((0,), (0,)), ((), ())), preferred_element_type=jnp.float32).astype(jnp.bfloat16)
        return (user_next, item_next, user_sum + user_next.astype(jnp.float32), item_sum + item_next.astype(jnp.float32)), None

    start_state = (user_emb, item_emb, user_emb.astype(jnp.float32), item_emb.astype(jnp.float32))
    end_state, unused_out = lax.scan(one_layer, start_state, None, length=LAYERS)
    final_user = (end_state[2] / (LAYERS + 1)).astype(jnp.bfloat16)
    final_item = (end_state[3] / (LAYERS + 1)).astype(jnp.bfloat16)
    picked = jnp.take(final_user, queries, axis=0)
    scores = lax.dot_general(picked, final_item, (((1,), (1,)), ((), ())), preferred_element_type=jnp.float32)
    return final_user, final_item, scores
```

```python
import jax
import jax.numpy as jnp
from jax import lax
from jax.experimental import pallas as pl
from jax.experimental.pallas import tpu as pltpu
from jax.sharding import PartitionSpec as P

MESH = pl.DeviceIdType.MESH
F32 = jnp.float32
BF16 = jnp.bfloat16
CHUNKS = 8
CHUNK = 512
HALF = 2048
ITEMS = 512
EMB = 64
ROWS = 64
OWN = 8


def peer_row(row, offset):
    peer = row
    for scale in (1, 4, 16):
        digit = (row // scale) % 4
        peer = peer + ((digit + (offset // scale) % 4) % 4 - digit) * scale
    return peer


def step_kernel(mask_hbm, user_ref, item_ref, query_ref, fuser_hbm, fitem_ref, score_ref,
                mask_i, mask_b, mask_o, adj, onehot, deg_src, deg_buf, deg_oth, item_src, item_buf, item0,
                part, pair_buf, red_src, red_buf, gat_src, gat_buf, item12, pick, fuser,
                load_sem, out_sem, send_sem, recv_sem):
    col = lax.axis_index('col')
    row = lax.axis_index('row')
    partner = (1 - col, row)

    loads = []
    for k in range(CHUNKS):
        first = (1 - col) * HALF if k < CHUNKS // 2 else col * HALF - HALF
        start = pl.multiple_of(first + k * CHUNK, CHUNK)
        loads.append(pltpu.make_async_copy(mask_hbm.at[pl.ds(start, CHUNK)], mask_i.at[pl.ds(k * CHUNK, CHUNK)], load_sem.at[k]))
        loads[-1].start()

    barrier = pltpu.get_barrier_semaphore()
    pl.semaphore_signal(barrier, inc=1, device_id=partner, device_id_type=MESH)

    def greet(e, carry):
        pl.semaphore_signal(barrier, inc=1, device_id=(col, peer_row(row, ROWS - e)), device_id_type=MESH)
        return carry
    lax.fori_loop(1, ROWS, greet, 0)

    def send_all(src, dst, sem):
        def one(e, carry):
            pltpu.make_async_remote_copy(src_ref=src, dst_ref=dst.at[row], send_sem=send_sem.at[sem], recv_sem=recv_sem.at[sem],
                                         device_id=(col, peer_row(row, ROWS - e)), device_id_type=MESH).start()
            return carry
        lax.fori_loop(1, ROWS, one, 0)

    def send_chunks(src, dst, sem):
        def one(e, carry):
            back = ROWS - e
            peer = peer_row(row, back)
            pltpu.make_async_remote_copy(src_ref=src.at[pl.ds(pl.multiple_of(peer * OWN, OWN), OWN)], dst_ref=dst.at[back - 1],
                                         send_sem=send_sem.at[sem], recv_sem=recv_sem.at[sem],
                                         device_id=(col, peer), device_id_type=MESH).start()
            return carry
        lax.fori_loop(1, ROWS, one, 0)

    def wait_recv(buf, sem):
        view = buf.at[pl.ds(0, ROWS - 1)]
        pltpu.make_async_copy(view, view, recv_sem.at[sem]).wait()

    def wait_sent(buf, sem):
        view = buf.at[pl.ds(0, ROWS - 1)]
        pltpu.make_async_copy(view, view, send_sem.at[sem]).wait()

    def to_partner(src, dst, sem):
        copy = pltpu.make_async_remote_copy(src_ref=src, dst_ref=dst, send_sem=send_sem.at[sem], recv_sem=recv_sem.at[sem],
                                            device_id=partner, device_id_type=MESH)
        copy.start()
        return copy

    own_item = item_ref[...].astype(F32)
    item_src[...] = jnp.concatenate([own_item, own_item], axis=1)

    count = jnp.zeros((8, ITEMS), jnp.int32)
    for k in range(CHUNKS):
        loads[k].wait()
        block = mask_i[pl.ds(k * CHUNK, CHUNK), :]
        count = count + jnp.sum(block.reshape(CHUNK // 8, 8, ITEMS), axis=0)
        mask_b[pl.ds(k * CHUNK, CHUNK), :] = block.astype(F32).astype(BF16)
    deg_own = jnp.sum(count, axis=0, keepdims=True)
    deg_src[...] = deg_own

    pl.semaphore_wait(barrier, ROWS)
    send_all(deg_src, deg_buf, 0)
    mask_copy = to_partner(mask_b.at[pl.ds(0, HALF)], mask_o, 1)
    send_all(item_src, item_buf, 2)

    query = query_ref[...]
    low, high = query[:, :ITEMS], query[:, ITEMS:]
    ordered = jnp.concatenate([jnp.where(col == 0, low, high), jnp.where(col == 0, high, low)], axis=1)
    local = ordered - (row * 2 + col) * HALF
    spread = jnp.transpose(jnp.broadcast_to(local, (128, 2 * ITEMS)))
    lane = lax.broadcasted_iota(jnp.int32, (2 * ITEMS, 128), 1)
    for k in range(HALF // 128):
        onehot[:, pl.ds(k * 128, 128)] = jnp.where(spread == lane + k * 128, 1.0, 0.0).astype(BF16)

    mask_copy.wait()
    ones = jnp.ones((ITEMS, 128), BF16)
    deg_user = (jnp.dot(mask_b[pl.ds(HALF, HALF), :], ones, preferred_element_type=F32)
                + jnp.dot(mask_o[...], ones, preferred_element_type=F32))
    inv_user = lax.rsqrt(jnp.maximum(deg_user, 1.0))

    wait_recv(item_buf, 2)
    item_buf[row] = item_src[...]
    item0[0] = item_buf[...].reshape(ITEMS, 128).astype(BF16)
    item_copy = to_partner(item0.at[0], item0.at[1], 3)

    wait_recv(deg_buf, 0)
    deg_buf[row] = deg_src[...]
    deg_item = jnp.sum(deg_buf[...], axis=0)
    wait_sent(deg_buf, 0)
    deg_src[...] = deg_item
    deg_copy = to_partner(deg_src, deg_oth, 4)

    def form(item_degree, mask_block, half):
        inv_item = lax.rsqrt(jnp.maximum(item_degree, 1).astype(F32))
        for k in range(ITEMS // 128):
            scale = (inv_user * inv_item[:, k * 128:(k + 1) * 128]).astype(BF16)
            adj[:, pl.ds(half * ITEMS + k * 128, 128)] = scale * mask_block[:, k * 128:(k + 1) * 128]

    form(deg_item, mask_b[pl.ds(HALF, HALF), :], 0)
    deg_copy.wait()
    form(deg_oth[...], mask_o[...], 1)
    item_copy.wait()

    user0 = user_ref[...]
    user1 = jnp.dot(adj[...], item0[...].reshape(2 * ITEMS, 128), preferred_element_type=F32).astype(BF16)
    user01 = jnp.concatenate([user0, user1[:, EMB:]], axis=1)

    def reduce_items(index):
        to_partner(part.at[pl.ds(ITEMS, ITEMS)], pair_buf.at[index], 5 + 4 * index).wait()
        red_src[index] = part[pl.ds(0, ITEMS), :] + pair_buf[index]
        send_chunks(red_src.at[index], red_buf.at[index], 6 + 4 * index)
        wait_recv(red_buf.at[index], 6 + 4 * index)
        total = red_src[index, pl.ds(pl.multiple_of(row * OWN, OWN), OWN), :] + jnp.sum(red_buf[index], axis=0)
        return total

    part[...] = jnp.transpose(jnp.dot(jnp.transpose(user01), adj[...], preferred_element_type=F32))
    own12 = reduce_items(0).astype(BF16).astype(F32)
    gat_src[0] = own12
    send_all(gat_src.at[0], gat_buf.at[0], 7)
    item_sum = (own_item + own12[:, :EMB]) + own12[:, EMB:]
    wait_recv(gat_buf.at[0], 7)
    gat_buf[0, row] = own12
    item12[0] = gat_buf[0].reshape(ITEMS, 128).astype(BF16)
    to_partner(item12.at[0], item12.at[1], 8).wait()

    user23 = jnp.dot(adj[...], item12[...].reshape(2 * ITEMS, 128), preferred_element_type=F32).astype(BF16)
    item3 = jnp.transpose(jnp.dot(jnp.transpose(user23[:, :EMB]), adj[...], preferred_element_type=F32))
    user_sum = ((user0.astype(F32) + user1[:, :EMB].astype(F32)) + user23[:, :EMB].astype(F32)) + user23[:, EMB:].astype(F32)
    final = (user_sum / 4.0).astype(BF16)
    fuser[...] = final
    out_copy = pltpu.make_async_copy(fuser, fuser_hbm, out_sem.at[0])
    out_copy.start()
    picked = jnp.dot(onehot[...], jnp.concatenate([final, final], axis=1), preferred_element_type=F32)
    part[...] = jnp.concatenate([item3, picked[:, EMB:]], axis=1)
    own3 = reduce_items(1)
    gat_src[1] = own3
    send_all(gat_src.at[1], gat_buf.at[1], 11)
    final_item = ((item_sum + own3[:, :EMB].astype(BF16).astype(F32)) / 4.0).astype(BF16)
    fitem_ref[...] = final_item
    weights = jnp.concatenate([jnp.zeros((OWN, EMB), BF16), final_item], axis=1)
    wait_recv(gat_buf.at[1], 11)
    gat_buf[1, row] = own3
    pick[0] = gat_buf[1].reshape(ITEMS, 128).astype(BF16)
    pick_copy = to_partner(pick.at[0], pick.at[1], 12)
    contract = (((1,), (1,)), ((), ()))
    score_ref[pl.ds(pl.multiple_of(col * ITEMS, ITEMS), ITEMS), :] = lax.dot_general(pick[0], weights, contract, preferred_element_type=F32)
    pick_copy.wait()
    score_ref[pl.ds(pl.multiple_of((1 - col) * ITEMS, ITEMS), ITEMS), :] = lax.dot_general(pick[1], weights, contract, preferred_element_type=F32)

    out_copy.wait()
    wait_sent(item_buf, 2)
    wait_sent(red_buf.at[0], 6)
    wait_sent(red_buf.at[1], 10)
    wait_sent(gat_buf.at[0], 7)
    wait_sent(gat_buf.at[1], 11)


def solution(mesh):
    vmem = pl.BlockSpec(memory_space=pltpu.VMEM)
    hbm = pl.BlockSpec(memory_space=pl.ANY)

    def device_step(mask_blk, user_shard, item_shard, queries):
        return pl.pallas_call(
            step_kernel,
            out_shape=(jax.ShapeDtypeStruct((HALF, EMB), BF16), jax.ShapeDtypeStruct((OWN, EMB), BF16),
                       jax.ShapeDtypeStruct((2 * ITEMS, OWN), F32)),
            in_specs=[hbm, vmem, vmem, vmem],
            out_specs=(hbm, vmem, vmem),
            scratch_shapes=[
                pltpu.VMEM((2 * HALF, ITEMS), jnp.int32),
                pltpu.VMEM((2 * HALF, ITEMS), BF16),
                pltpu.VMEM((HALF, ITEMS), BF16),
                pltpu.VMEM((HALF, 2 * ITEMS), BF16),
                pltpu.VMEM((2 * ITEMS, HALF), BF16),
                pltpu.VMEM((1, ITEMS), jnp.int32),
                pltpu.VMEM((ROWS, 1, ITEMS), jnp.int32),
                pltpu.VMEM((1, ITEMS), jnp.int32),
                pltpu.VMEM((OWN, 128), F32),
                pltpu.VMEM((ROWS, OWN, 128), F32),
                pltpu.VMEM((2, ITEMS, 128), BF16),
                pltpu.VMEM((2 * ITEMS, 128), F32),
                pltpu.VMEM((2, ITEMS, 128), F32),
                pltpu.VMEM((2, ITEMS, 128), F32),
                pltpu.VMEM((2, ROWS - 1, OWN, 128), F32),
                pltpu.VMEM((2, OWN, 128), F32),
                pltpu.VMEM((2, ROWS, OWN, 128), F32),
                pltpu.VMEM((2, ITEMS, 128), BF16),
                pltpu.VMEM((2, ITEMS, 128), BF16),
                pltpu.VMEM((HALF, EMB), BF16),
                pltpu.SemaphoreType.DMA((CHUNKS,)),
                pltpu.SemaphoreType.DMA((1,)),
                pltpu.SemaphoreType.DMA((13,)),
                pltpu.SemaphoreType.DMA((13,)),
            ],
            compiler_params=pltpu.CompilerParams(collective_id=0, has_side_effects=True, vmem_limit_bytes=60 * 1024 * 1024),
        )(mask_blk, user_shard, item_shard, queries.reshape(1, 2 * ITEMS))

    return jax.shard_map(device_step, mesh=mesh, in_specs=(P('row', 'col'), P(('row', 'col'), None), P(('col', 'row'), None), P()),
                         out_specs=(P(('row', 'col'), None), P(('col', 'row'), None), P(None, ('col', 'row'))), check_vma=False)
```

```python
import jax
import jax.numpy as jnp
from jax import lax
from jax.experimental import pallas as pl
from jax.experimental.pallas import tpu as pltpu
from jax.sharding import PartitionSpec as P

MESH = pl.DeviceIdType.MESH
F32 = jnp.float32
BF16 = jnp.bfloat16
CHUNKS = 8
CHUNK = 512
HALF = 2048
ITEMS = 512
ALL_ITEMS = 1024
EMB = 64
ROWS = 64
OWN = 8
HOPS = (0, 1, 2, 1)
LAST = (((1,), (1,)), ((), ()))

PLACES = [(p, z, y, x) for p in range(2) for z in range(4) for y in range(4) for x in range(4)][1:]
PLACES.sort(key=lambda place: (-sum(HOPS[d] for d in place[1:]), place))
SAME_CORE = [place for place in PLACES if place[0] == 0]
LINE_X = [(0, 0, 0, d) for d in (2, 1, 3)]
LINE_Y = [(0, 0, d, 0) for d in (2, 1, 3)]
LINE_Z = [(p, d, 0, 0) for d in (2, 1, 3, 0) for p in (1, 0) if p or d]


def step_kernel(mask_hbm, user_hbm, item_hbm, query_hbm, fuser_out, fitem_out, score_out,
                mask_i, mask_b, mask_o, adj, onehot, inv_user, user01, item_own, query, deg_src, deg_x, deg_y, deg_z,
                item_src, item_pair, item_quad, item_x, item_y, item_z,
                part, pair_buf, red_src, red_buf, gat_src, gat_buf, pick_src, pick_buf, fuser, fitem, score,
                load_sem, in_sem, out_sem, send_sem, recv_sem):
    col = lax.axis_index('col')
    row = lax.axis_index('row')
    at_x, at_y, at_z = row % 4, (row // 4) % 4, row // 16
    xs = [(at_x + d) % 4 for d in range(4)]
    ys = [((at_y + d) % 4) * 4 for d in range(4)]
    zs = [((at_z + d) % 4) * 16 for d in range(4)]
    cols = [col, 1 - col]
    partner = (1 - col, row)

    def device(place):
        p, z, y, x = place
        return cols[p], zs[z] + ys[y] + xs[x]

    loads = []
    for k in range(CHUNKS):
        first = (1 - col) * HALF if k < CHUNKS // 2 else col * HALF - HALF
        start = pl.multiple_of(first + k * CHUNK, CHUNK)
        loads.append(pltpu.make_async_copy(mask_hbm.at[pl.ds(start, CHUNK)], mask_i.at[pl.ds(k * CHUNK, CHUNK)], load_sem.at[k]))
        loads[-1].start()
    small = [pltpu.make_async_copy(item_hbm, item_own, in_sem.at[0]), pltpu.make_async_copy(query_hbm, query, in_sem.at[1]),
             pltpu.make_async_copy(user_hbm, user01.at[pl.ds(0, EMB)], in_sem.at[2])]
    for copy in small:
        copy.start()

    with jax.named_scope('greet'):
        barrier = pltpu.get_barrier_semaphore()
        for place in LINE_X + LINE_Y + LINE_Z:
            pl.semaphore_signal(barrier, inc=1, device_id=device(place), device_id_type=MESH)

    def send_to(places, src, dst, sem):
        for place in places:
            pltpu.make_async_remote_copy(src_ref=src, dst_ref=dst, send_sem=send_sem.at[sem], recv_sem=recv_sem.at[sem],
                                         device_id=device(place), device_id_type=MESH).start()

    def send_chunks(src, dst, sem):
        for n, place in enumerate(SAME_CORE):
            target = device(place)
            rows = pl.ds(pl.multiple_of(target[1] * OWN, OWN), OWN)
            pltpu.make_async_remote_copy(src_ref=src.at[rows], dst_ref=dst.at[n], send_sem=send_sem.at[sem], recv_sem=recv_sem.at[sem],
                                         device_id=target, device_id_type=MESH).start()

    def wait_slots(buf, sem, slots):
        view = buf.at[pl.ds(0, slots)]
        pltpu.make_async_copy(view, view, sem).wait()

    def to_partner(src, dst, sem):
        copy = pltpu.make_async_remote_copy(src_ref=src, dst_ref=dst, send_sem=send_sem.at[sem], recv_sem=recv_sem.at[sem],
                                            device_id=partner, device_id_type=MESH)
        copy.start()
        return copy

    with jax.named_scope('load'):
        small[0].wait()
        own_item = item_own[...]
        item_src[...] = jnp.concatenate([own_item, own_item], axis=1)
        count = jnp.zeros((8, ITEMS), jnp.int32)
        for k in range(CHUNKS):
            loads[k].wait()
            block = mask_i[pl.ds(k * CHUNK, CHUNK), :]
            count = count + jnp.sum(block.reshape(CHUNK // 8, 8, ITEMS), axis=0)
            mask_b[pl.ds(k * CHUNK, CHUNK), :] = block.astype(F32).astype(BF16)
        deg_src[0] = jnp.sum(count, axis=0, keepdims=True)
    with jax.named_scope('barrier'):
        pl.semaphore_wait(barrier, len(LINE_X + LINE_Y + LINE_Z))

    lower = lax.broadcasted_iota(jnp.int32, (OWN, 128), 1) < EMB
    with jax.named_scope('send_x'):
        send_to(LINE_X, deg_src.at[0], deg_x.at[at_x], 0)
        send_to(LINE_X, item_src, item_x.at[at_x], 2)
        mask_copy = to_partner(mask_b.at[pl.ds(0, HALF)], mask_o, 1)

    with jax.named_scope('onehot'):
        small[1].wait()
        ids = query[...]
        low, high = ids[:, :ITEMS], ids[:, ITEMS:]
        ordered = jnp.concatenate([jnp.where(col == 0, low, high), jnp.where(col == 0, high, low)], axis=1)
        local = jnp.broadcast_to(ordered - (row * 2 + col) * HALF, (128, ALL_ITEMS))
        place_in = lax.broadcasted_iota(jnp.int32, (128, ALL_ITEMS), 0)
        for k in range(HALF // 128):
            onehot[pl.ds(k * 128, 128), :] = jnp.where(local == place_in + k * 128, 1.0, 0.0).astype(BF16)

    with jax.named_scope('wait_x'):
        wait_slots(deg_x, recv_sem.at[0], 3)
        deg_x[at_x] = deg_src[0]
        deg_src[1] = jnp.sum(deg_x[...], axis=0)
        send_to(LINE_Y, deg_src.at[1], deg_y.at[at_y], 9)
    with jax.named_scope('wait_x2'):
        wait_slots(item_x, recv_sem.at[2], 3)
        item_x[at_x] = item_src[...]
        for n in range(2):
            item_pair[n] = jnp.where(lower, item_x[2 * n].astype(F32), item_x[2 * n + 1].astype(F32)).astype(BF16)
        send_to(LINE_Y, item_pair, item_y.at[at_y], 10)

    with jax.named_scope('mask_wait'):
        mask_copy.wait()
    with jax.named_scope('deg_user'):
        ones = jnp.ones((ITEMS, 128), BF16)
        deg_user = (jnp.dot(mask_b[pl.ds(HALF, HALF), :], ones, preferred_element_type=F32)
                    + jnp.dot(mask_o[...], ones, preferred_element_type=F32))
        inv_user[...] = lax.rsqrt(jnp.maximum(deg_user, 1.0))

    with jax.named_scope('wait_y'):
        wait_slots(deg_y, recv_sem.at[9], 3)
        deg_y[at_y] = deg_src[1]
        deg_src[2] = jnp.sum(deg_y[...], axis=0)
        send_to(LINE_Z, deg_src.at[2], deg_z.at[col * 4 + at_z], 11)
    with jax.named_scope('wait_y2'):
        wait_slots(item_y, recv_sem.at[10], 3)
        item_y[at_y] = item_pair[...]
        item_quad[...] = item_y[...]
        send_to(LINE_Z, item_quad, item_z.at[col * 4 + at_z], 12)
        small[2].wait()

    def own_first(buf):
        return jnp.where(col == 0, buf[0], buf[1]), jnp.where(col == 0, buf[1], buf[0])

    with jax.named_scope('wait_z'):
        wait_slots(deg_z, recv_sem.at[11], 7)
        deg_z[col * 4 + at_z] = deg_src[2]
        deg_all = own_first(jnp.sum(deg_z[...].reshape(2, 4, 1, ITEMS), axis=1))
        inv_item = [lax.rsqrt(jnp.maximum(deg, 1).astype(F32)) for deg in deg_all]

    def form(chunk):
        for half in range(2):
            rows = pl.ds(chunk * CHUNK, CHUNK)
            block = mask_b[pl.ds(HALF + chunk * CHUNK, CHUNK), :] if half == 0 else mask_o[rows, :]
            for k in range(ITEMS // 128):
                scale = (inv_user[rows, :] * inv_item[half][:, k * 128:(k + 1) * 128]).astype(BF16)
                adj[rows, pl.ds(half * ITEMS + k * 128, 128)] = scale * block[:, k * 128:(k + 1) * 128]

    with jax.named_scope('form0'):
        form(0)
    with jax.named_scope('wait_item0'):
        wait_slots(item_z, recv_sem.at[12], 7)
        item_z[col * 4 + at_z] = item_quad[...]
        packed = item_z[...].astype(F32)
        turned = pltpu.roll(packed.reshape(64 * OWN, 128), EMB, 1).reshape(packed.shape)
        rows = jnp.stack([packed, turned], axis=3).reshape(2, ITEMS, 128)
        item0 = jnp.concatenate([jnp.transpose(half)[:EMB] for half in own_first(rows)], axis=1).astype(BF16)
    with jax.named_scope('m1'):
        for k in range(HALF // CHUNK):
            if k:
                form(k)
            user1 = lax.dot_general(item0, adj[pl.ds(k * CHUNK, CHUNK), :], LAST, preferred_element_type=F32).astype(BF16)
            user01[pl.ds(EMB, EMB), pl.ds(k * CHUNK, CHUNK)] = user1

    def reduce_items(index, make):
        with jax.named_scope('make%d' % index):
            part[1] = make(1)
            copy = to_partner(part.at[1], pair_buf.at[index], 3 + 3 * index)
            part[0] = make(0)
        with jax.named_scope('pair%d' % index):
            copy.wait()
            red_src[index] = part[0] + pair_buf[index]
        with jax.named_scope('send_red%d' % index):
            send_chunks(red_src.at[index], red_buf.at[index], 4 + 3 * index)

    def reduced(index):
        with jax.named_scope('wait_red%d' % index):
            wait_slots(red_buf.at[index], recv_sem.at[4 + 3 * index], ROWS - 1)
        return red_src[index, pl.ds(pl.multiple_of(row * OWN, OWN), OWN), :] + jnp.sum(red_buf[index], axis=0)

    reduce_items(0, lambda half: jnp.transpose(jnp.dot(user01[...], adj[:, half * ITEMS:(half + 1) * ITEMS], preferred_element_type=F32)))
    own12 = reduced(0).astype(BF16)
    with jax.named_scope('send_gat'):
        gat_src[...] = own12
        send_to(PLACES, gat_src, gat_buf.at[col * ROWS + row], 5)
    item_sum = (own_item.astype(F32) + own12[:, :EMB].astype(F32)) + own12[:, EMB:].astype(F32)
    with jax.named_scope('wait_gat'):
        wait_slots(gat_buf, recv_sem.at[5], 2 * ROWS - 1)
        gat_buf[col * ROWS + row] = own12
    with jax.named_scope('t12'):
        rows = gat_buf[...].astype(F32).reshape(2, ITEMS, 128)
        item12 = jnp.concatenate([jnp.transpose(half) for half in own_first(rows)], axis=1).astype(BF16)
    with jax.named_scope('m3'):
        user23 = lax.dot_general(item12, adj[...], LAST, preferred_element_type=F32).astype(BF16)
        user_sum = (user01[:EMB, :].astype(F32) + user01[EMB:, :].astype(F32)) + user23[:EMB].astype(F32)
        final = ((user_sum + user23[EMB:].astype(F32)) / 4.0).astype(BF16)
        fuser[...] = final
    out_copy = pltpu.make_async_copy(fuser, fuser_out, out_sem.at[0])
    out_copy.start()

    def item3_and_picks(half):
        cut = slice(half * ITEMS, (half + 1) * ITEMS)
        item3 = jnp.dot(user23[:EMB], adj[:, cut], preferred_element_type=F32)
        picked = jnp.dot(final, onehot[:, cut], preferred_element_type=F32)
        return jnp.transpose(jnp.concatenate([item3, picked], axis=0))

    reduce_items(1, item3_and_picks)
    own3 = reduced(1)
    with jax.named_scope('send_pick'):
        pick_src[...] = own3.astype(BF16)
        send_to(PLACES, pick_src, pick_buf.at[col * ROWS + row], 8)
    final_item = ((item_sum + own3[:, :EMB].astype(BF16).astype(F32)) / 4.0).astype(BF16)
    fitem[...] = final_item
    weights = jnp.concatenate([jnp.zeros((OWN, EMB), BF16), final_item], axis=1)
    with jax.named_scope('wait_pick'):
        wait_slots(pick_buf, recv_sem.at[8], 2 * ROWS - 1)
        pick_buf[col * ROWS + row] = pick_src[...]
    with jax.named_scope('score'):
        rows = pick_buf[...].astype(F32).reshape(ALL_ITEMS, 128).astype(BF16)
        score[...] = lax.dot_general(weights, rows, LAST, preferred_element_type=F32)
    with jax.named_scope('finish'):
        outs = [pltpu.make_async_copy(fitem, fitem_out, out_sem.at[1]), pltpu.make_async_copy(score, score_out, out_sem.at[2])]
        for copy in outs:
            copy.start()
        for buf, sem, slots in ((deg_x, 0, 3), (deg_y, 9, 3), (deg_z, 11, 7), (item_x, 2, 3), (item_y, 10, 3), (item_z, 12, 7),
                                (red_buf.at[0], 4, ROWS - 1), (gat_buf, 5, 2 * ROWS - 1), (red_buf.at[1], 7, ROWS - 1),
                                (pick_buf, 8, 2 * ROWS - 1)):
            wait_slots(buf, send_sem.at[sem], slots)
        out_copy.wait()
        for copy in outs:
            copy.wait()


def hand_over(fuser_in, fitem_in, score_in, fuser_out, fitem_out, score_out):
    fuser_out[...] = fuser_in[...]
    fitem_out[...] = fitem_in[...]
    score_out[...] = score_in[...]


def solution(mesh):
    hbm = pl.BlockSpec(memory_space=pl.ANY)
    vmem = pl.BlockSpec(memory_space=pltpu.VMEM)
    shapes = (jax.ShapeDtypeStruct((EMB, HALF), BF16), jax.ShapeDtypeStruct((OWN, EMB), BF16), jax.ShapeDtypeStruct((OWN, ALL_ITEMS), F32))

    def device_step(mask_blk, user_shard, item_shard, queries):
        outs = pl.pallas_call(
            step_kernel,
            out_shape=shapes,
            in_specs=[hbm, hbm, hbm, hbm],
            out_specs=(hbm, hbm, hbm),
            scratch_shapes=[
                pltpu.VMEM((2 * HALF, ITEMS), jnp.int32),
                pltpu.VMEM((2 * HALF, ITEMS), BF16),
                pltpu.VMEM((HALF, ITEMS), BF16),
                pltpu.VMEM((HALF, ALL_ITEMS), BF16),
                pltpu.VMEM((HALF, ALL_ITEMS), BF16),
                pltpu.VMEM((HALF, 128), F32),
                pltpu.VMEM((2 * EMB, HALF), BF16),
                pltpu.VMEM((OWN, EMB), BF16),
                pltpu.VMEM((1, ALL_ITEMS), jnp.int32),
                pltpu.VMEM((3, 1, ITEMS), jnp.int32),
                pltpu.VMEM((4, 1, ITEMS), jnp.int32),
                pltpu.VMEM((4, 1, ITEMS), jnp.int32),
                pltpu.VMEM((8, 1, ITEMS), jnp.int32),
                pltpu.VMEM((OWN, 128), BF16),
                pltpu.VMEM((2, OWN, 128), BF16),
                pltpu.VMEM((4, 2, OWN, 128), BF16),
                pltpu.VMEM((4, OWN, 128), BF16),
                pltpu.VMEM((4, 2, OWN, 128), BF16),
                pltpu.VMEM((8, 4, 2, OWN, 128), BF16),
                pltpu.VMEM((2, ITEMS, 128), F32),
                pltpu.VMEM((2, ITEMS, 128), F32),
                pltpu.VMEM((2, ITEMS, 128), F32),
                pltpu.VMEM((2, ROWS - 1, OWN, 128), F32),
                pltpu.VMEM((OWN, 128), BF16),
                pltpu.VMEM((2 * ROWS, OWN, 128), BF16),
                pltpu.VMEM((OWN, 128), BF16),
                pltpu.VMEM((2 * ROWS, OWN, 128), BF16),
                pltpu.VMEM((EMB, HALF), BF16),
                pltpu.VMEM((OWN, EMB), BF16),
                pltpu.VMEM((OWN, ALL_ITEMS), F32),
                pltpu.SemaphoreType.DMA((CHUNKS,)),
                pltpu.SemaphoreType.DMA((3,)),
                pltpu.SemaphoreType.DMA((3,)),
                pltpu.SemaphoreType.DMA((13,)),
                pltpu.SemaphoreType.DMA((13,)),
            ],
            compiler_params=pltpu.CompilerParams(collective_id=0, has_side_effects=True, vmem_limit_bytes=60 * 1024 * 1024),
        )(mask_blk, user_shard.T, item_shard, queries.reshape(1, ALL_ITEMS))
        fuser, fitem, score = pl.pallas_call(hand_over, out_shape=shapes, in_specs=[vmem] * 3, out_specs=(vmem,) * 3)(*outs)
        return fuser.T, fitem, score.T

    return jax.shard_map(device_step, mesh=mesh, in_specs=(P('row', 'col'), P(('row', 'col'), None), P(('col', 'row'), None), P()),
                         out_specs=(P(('row', 'col'), None), P(('col', 'row'), None), P(None, ('col', 'row'))), check_vma=False)
```
